256 devices in a mesh: ta: 8 (over x, z_lo), sa: 32 (over z_hi, y, core).
Axes of the slice: x: 4, y: 4, z: 8 (z_hi: 4, z_lo: 2; z = z_hi * 2 + z_lo), core: 2. Of those that a mesh axis runs over, the one named last changes fastest.
Arguments:
- eigvecs: bfloat16 [48, 2, 3, 13824, 128], P('ta', None, None, 'sa'), may hold values from -0.0390625 to 0.0390625
- solutions: bfloat16 [48, 2, 3, 13824, 128], P('ta', None, None, 'sa'), may hold values from -6 to 6
Outputs:
- tau: float32 [48, 2, 128, 128], P('ta', None, 'sa')
- corr: float32 [48], replicated
The draws below stay inside these ranges and needn't reach their ends.
All inputs are finite; a program needn't handle non-finite values.
Results may differ from the reference program's by a relative error of at most 0.0003.
Values sent between devices are 32-bit elements; how exact they have to be, the bound alone decides.
No kernel may reach another device: no remote copies, remote signals or barrier semaphores. Data moves between devices by JAX's collectives and lax.ppermute only.
A program may use at most 64 MiB of HBM per device.

```python
import jax
import jax.numpy as jnp
from jax import lax

NEV = 128
NB = 128
NT = 48
SITES = 13824


def strengthened(entries, stream_key, source, target, parts, factor):
    def block_of(position):
        return (jnp.arange(entries.shape[position]) // (entries.shape[position] // parts)).reshape((-1,) + (1,) * (entries.ndim - 1 - position))

    near = jax.random.permutation(stream_key, parts)[block_of(target)]
    second = (block_of(target) + parts // 2) % parts
    return jnp.where((block_of(source) == near) | (block_of(source) == second), factor * entries, entries)


def steps_of(own_key, dims, split, smallest, top_value):
    loudness = 1.0
    for position, blocks in split:
        draws = jax.random.uniform(jax.random.fold_in(jax.random.fold_in(own_key, 6), position), (blocks,), jnp.float32, smallest / len(split), top_value / len(split))
        loudness = loudness * jnp.repeat(jnp.exp(draws), dims[position] // blocks).reshape((-1,) + (1,) * (len(dims) - 1 - position))
    return loudness


def bell_draw(stream_key, extent, deviation, reach, cuts=(), kind=jnp.bfloat16):
    drawn = deviation * jax.random.normal(stream_key, extent, jnp.float32)
    if cuts:
        drawn = drawn * steps_of(stream_key, extent, cuts, -0.22, 0.18)
    return jnp.clip(drawn, -reach, reach).astype(kind)


def gaussian_with(own_key, dims, width, bound, shards, heavy, dtype=jnp.bfloat16):
    drawn = width * jax.random.normal(own_key, dims, jnp.float32)
    if shards:
        drawn = drawn * steps_of(own_key, dims, shards, -0.22, 0.18)
    return jnp.clip(strengthened(drawn, jax.random.fold_in(own_key, 3), *heavy), -bound, bound).astype(dtype)


def setup_inputs(seed: int = 0) -> dict:
    splits = jax.random.split(jax.random.key(seed), 3)
    return {
        "eigvecs": gaussian_with(splits[0], (NT, 2, 3, SITES, NEV), (6 * SITES) ** -0.5, 0.0390625, ((0, 8), (3, 32)), (3, 4, 32, 2.75)),
        "solutions": bell_draw(splits[1], (NT, 2, 3, SITES, NB), 1.0, 6.0, ((0, 8), (3, 32))),
    }


def contract(left, right):
    return lax.dot_general(left, right, (((0,), (0,)), ((), ())), preferred_element_type=jnp.float32)


def one_slice(pair):
    vecs, sols = pair
    vec_re = vecs[0].reshape(-1, vecs.shape[-1])
    vec_im = vecs[1].reshape(-1, vecs.shape[-1])
    sol_re = sols[0].reshape(-1, sols.shape[-1])
    sol_im = sols[1].reshape(-1, sols.shape[-1])
    real_part = contract(vec_re, sol_re) + contract(vec_im, sol_im)
    imag_part = contract(vec_re, sol_im) - contract(vec_im, sol_re)
    return jnp.stack([real_part, imag_part], 0)


def reference(eigvecs, solutions):
    tau = lax.map(one_slice, (eigvecs, solutions))
    corr = jnp.sum(tau * tau, axis=(1, 2, 3)) / (2.0 * NEV * NB)
    return tau, corr
```

```python
import jax
import jax.numpy as jnp
from jax import lax
from jax.sharding import Mesh, PartitionSpec as P

AXES = ("x", "zl", "zh", "y", "core")
SIZES = (4, 2, 4, 4, 2)
TA = ("x", "zl")
SA = ("zh", "y", "core")


def shifted(array, axis, by):
    length = lax.axis_size(axis)
    return lax.ppermute(array, axis, [(i, (i + by) % length) for i in range(length)])


def block_at(blocks, index):
    return lax.dynamic_index_in_dim(blocks, index, 0, keepdims=False)


def sum_at_owner(blocks, axis):
    length = lax.axis_size(axis)
    me = lax.axis_index(axis)
    total = block_at(blocks, me)
    for by in range(1, length):
        total = total + shifted(block_at(blocks, (me + by) % length), axis, by)
    return total


def per_device(eigvecs, solutions):
    slices = eigvecs.shape[0]
    vec_re = eigvecs[:, 0].reshape(slices, -1, eigvecs.shape[-1])
    vec_im = eigvecs[:, 1].reshape(slices, -1, eigvecs.shape[-1])
    sol_re = solutions[:, 0].reshape(slices, -1, solutions.shape[-1])
    sol_im = solutions[:, 1].reshape(slices, -1, solutions.shape[-1])

    def contract(left, right):
        return jnp.einsum("tka,tkb->tab", left, right, preferred_element_type=jnp.float32)

    real_part = contract(vec_re, sol_re) + contract(vec_im, sol_im)
    imag_part = contract(vec_re, sol_im) - contract(vec_im, sol_re)
    partial_tau = jnp.stack([real_part, imag_part], 1)
    rows, columns = partial_tau.shape[2:]
    scale = 1.0 / (2.0 * rows * columns)
    zh, y, core = (lax.axis_size(axis) for axis in SA)
    half = slices // core
    block = rows // (zh * y)
    tiles = partial_tau.reshape(core, half, 2, zh, y, block, columns)
    tiles = jnp.transpose(tiles, (0, 4, 3, 1, 2, 5, 6))
    tiles = sum_at_owner(tiles, "core")
    tiles = sum_at_owner(tiles, "y")
    mine = sum_at_owner(tiles, "zh")
    norms = jnp.sum(mine * mine, axis=(1, 2, 3))
    chips = ("x", "zl", "zh", "y")
    count = 1
    for axis in chips:
        count *= lax.axis_size(axis)
    copies = jnp.broadcast_to(norms, (count, 1, half))
    gathered = lax.all_to_all(copies, chips, split_axis=0, concat_axis=0, tiled=True)
    corr_half = jnp.sum(gathered.reshape(-1, zh * y, half), axis=1) * scale
    me = lax.axis_index("core")
    pieces = jnp.moveaxis(mine.reshape(half, 2, core, block // core, columns), 2, 0)
    kept = block_at(pieces, me)
    received = shifted(block_at(pieces, 1 - me), "core", 1)
    corr_other = shifted(corr_half, "core", 1)

    def in_order(own, other):
        return jnp.where(me == 0, jnp.stack([own, other]), jnp.stack([other, own]))

    tau = in_order(kept, received).reshape(slices, 2, block // core, columns)
    corr = jnp.moveaxis(in_order(corr_half, corr_other), 0, 1).reshape(-1)
    return (tau, corr)


def solution(mesh):
    fine = Mesh(mesh.devices.reshape(SIZES), AXES)
    in_specs = (P(TA, None, None, SA, None), P(TA, None, None, SA, None))
    out_specs = (P(TA, None, SA, None), P())
    return jax.shard_map(
        per_device, mesh=fine, in_specs=in_specs, out_specs=out_specs, check_vma=False
    )
```

```python
import functools

import jax
import jax.numpy as jnp
from jax import lax
from jax.experimental import pallas as pl
from jax.experimental.pallas import tpu as pltpu
from jax.sharding import Mesh, PartitionSpec as P

AXES = ("x", "zl", "zh", "y", "core")
SIZES = (4, 2, 4, 4, 2)
TA = ("x", "zl")
SA = ("zh", "y", "core")
CHIPS = ("x", "zl", "zh", "y")


def project_kernel(partner, vecs, sols, out, vec_buf, sol_buf, sems):
    half = out.shape[2]
    owner = lax.axis_index("core")
    if partner:
        owner = 1 - owner
    copies = []
    for i in range(half):
        t = owner * half + i
        pair = [
            pltpu.make_async_copy(vecs.at[t], vec_buf.at[i], sems.at[0, i]),
            pltpu.make_async_copy(sols.at[t], sol_buf.at[i], sems.at[1, i]),
        ]
        for copy in pair:
            copy.start()
        copies.append(pair)
    ny, nz = out.shape[:2]
    rows = out.shape[4]
    for i in range(half):
        for copy in copies[i]:
            copy.wait()
        depth = vec_buf.shape[2] * vec_buf.shape[3]
        nev, nb = vec_buf.shape[-1], sol_buf.shape[-1]
        left = jnp.concatenate([vec_buf[i, p].reshape(depth, nev) for p in range(2)], 1)
        right = jnp.concatenate([sol_buf[i, p].reshape(depth, nb) for p in range(2)], 1)
        product = lax.dot_general(
            left, right, (((0,), (0,)), ((), ())), preferred_element_type=jnp.float32
        )
        real = product[:nev, :nb] + product[nev:, nb:]
        imag = product[:nev, nb:] - product[nev:, :nb]
        for z in range(nz):
            for y in range(ny):
                at = (z * ny + y) * rows
                out[y, z, i, 0] = real[at : at + rows]
                out[y, z, i, 1] = imag[at : at + rows]


def project(eigvecs, solutions, partner):
    zh, y, core = (lax.axis_size(axis) for axis in SA)
    half = eigvecs.shape[0] // core
    rows = eigvecs.shape[-1] // (zh * y)
    columns = solutions.shape[-1]
    return pl.pallas_call(
        functools.partial(project_kernel, partner),
        out_shape=pltpu.VMEM((y, zh, half, 2, rows, columns), jnp.float32),
        in_specs=[pl.BlockSpec(memory_space=pltpu.HBM)] * 2,
        out_specs=pl.BlockSpec(memory_space=pltpu.VMEM),
        scratch_shapes=[
            pltpu.VMEM((half, *eigvecs.shape[1:]), eigvecs.dtype),
            pltpu.VMEM((half, *solutions.shape[1:]), solutions.dtype),
            pltpu.SemaphoreType.DMA((2, half)),
        ],
        cost_estimate=pl.CostEstimate(
            flops=half * 8 * eigvecs[0, 0].size * columns,
            bytes_accessed=eigvecs.size * 2,
            transcendentals=0,
        ),
        compiler_params=pltpu.CompilerParams(vmem_limit_bytes=16 << 20),
        name="project_partner" if partner else "project_own",
    )(
        pltpu.with_memory_space_constraint(eigvecs, pltpu.HBM),
        pltpu.with_memory_space_constraint(solutions, pltpu.HBM),
    )


def shifted(array, axis, by):
    length = lax.axis_size(axis)
    return lax.ppermute(array, axis, [(i, (i + by) % length) for i in range(length)])


def block_at(blocks, index):
    return lax.dynamic_index_in_dim(blocks, index, 0, keepdims=False)


def sum_at_owner(blocks, axis):
    length = lax.axis_size(axis)
    me = lax.axis_index(axis)
    total = block_at(blocks, me)
    for by in range(1, length):
        total = total + shifted(block_at(blocks, (me + by) % length), axis, by)
    return total


def per_device(eigvecs, solutions):
    zh, y, core = (lax.axis_size(axis) for axis in SA)
    rows, columns = eigvecs.shape[-1], solutions.shape[-1]
    scale = 1.0 / (2.0 * rows * columns)
    slices = eigvecs.shape[0]
    half = slices // core
    block = rows // (zh * y)
    from_partner = shifted(project(eigvecs, solutions, True), "core", 1)
    tiles = project(eigvecs, solutions, False) + from_partner
    tiles = sum_at_owner(tiles, "y")
    mine = sum_at_owner(tiles, "zh")
    norms = jnp.sum(mine * mine, axis=(1, 2, 3))
    count = 1
    for axis in CHIPS:
        count *= lax.axis_size(axis)
    copies = jnp.broadcast_to(norms, (count, 1, half))
    copies, mine, me = lax.optimization_barrier((copies, mine, lax.axis_index("core")))
    gathered = lax.all_to_all(copies, CHIPS, split_axis=0, concat_axis=0, tiled=True)
    gathered, mine, me = lax.optimization_barrier((gathered, mine, me))
    pieces = jnp.moveaxis(mine.reshape(half, 2, core, block // core, columns), 2, 0)
    kept = block_at(pieces, me)
    received = shifted(block_at(pieces, 1 - me), "core", 1)
    corr_half = jnp.sum(gathered.reshape(-1, zh * y, half), axis=1) * scale
    corr_other = shifted(corr_half, "core", 1)

    def in_order(own, other):
        return jnp.where(me == 0, jnp.stack([own, other]), jnp.stack([other, own]))

    tau = in_order(kept, received).reshape(slices, 2, block // core, columns)
    corr = jnp.moveaxis(in_order(corr_half, corr_other), 0, 1).reshape(-1)
    return (tau, corr)


def solution(mesh):
    fine = Mesh(mesh.devices.reshape(SIZES), AXES)
    in_specs = (P(TA, None, None, SA, None), P(TA, None, None, SA, None))
    out_specs = (P(TA, None, SA, None), P())
    return jax.shard_map(
        per_device, mesh=fine, in_specs=in_specs, out_specs=out_specs, check_vma=False
    )
```

```python
import functools

import jax
import jax.numpy as jnp
from jax import lax
from jax.experimental import pallas as pl
from jax.experimental.pallas import tpu as pltpu
from jax.sharding import Mesh, PartitionSpec as P

AXES = ("x", "zl", "zq", "zp", "y", "core")
SIZES = (4, 2, 2, 2, 4, 2)
TA = ("x", "zl")
SA = ("zq", "zp", "y", "core")
CHIPS = ("x", "zl", "y")


def project_kernel(partner, vecs, sols, out, vec_buf, sol_buf, sems):
    half = out.shape[2]
    owner = lax.axis_index("core")
    if partner:
        owner = 1 - owner
    copies = []
    for i in range(half):
        t = owner * half + i
        pair = [
            pltpu.make_async_copy(vecs.at[t], vec_buf.at[i], sems.at[0, i]),
            pltpu.make_async_copy(sols.at[t], sol_buf.at[i], sems.at[1, i]),
        ]
        for copy in pair:
            copy.start()
        copies.append(pair)
    ny, nz = out.shape[:2]
    rows = out.shape[4]
    for i in range(half):
        for copy in copies[i]:
            copy.wait()
        depth = vec_buf.shape[2] * vec_buf.shape[3]
        nev, nb = vec_buf.shape[-1], sol_buf.shape[-1]
        left = jnp.concatenate([vec_buf[i, p].reshape(depth, nev) for p in range(2)], 1)
        right = jnp.concatenate([sol_buf[i, p].reshape(depth, nb) for p in range(2)], 1)
        product = lax.dot_general(
            left, right, (((0,), (0,)), ((), ())), preferred_element_type=jnp.float32
        )
        real = product[:nev, :nb] + product[nev:, nb:]
        imag = product[:nev, nb:] - product[nev:, :nb]
        for z in range(nz):
            for y in range(ny):
                at = (z * ny + y) * rows
                out[y, z, i, 0] = real[at : at + rows]
                out[y, z, i, 1] = imag[at : at + rows]


def project(eigvecs, solutions, partner):
    zq, zp, y, core = (lax.axis_size(axis) for axis in SA)
    zh = zq * zp
    half = eigvecs.shape[0] // core
    rows = eigvecs.shape[-1] // (zh * y)
    columns = solutions.shape[-1]
    return pl.pallas_call(
        functools.partial(project_kernel, partner),
        out_shape=pltpu.VMEM((y, zh, half, 2, rows, columns), jnp.float32),
        in_specs=[pl.BlockSpec(memory_space=pltpu.HBM)] * 2,
        out_specs=pl.BlockSpec(memory_space=pltpu.VMEM),
        scratch_shapes=[
            pltpu.VMEM((half, *eigvecs.shape[1:]), eigvecs.dtype),
            pltpu.VMEM((half, *solutions.shape[1:]), solutions.dtype),
            pltpu.SemaphoreType.DMA((2, half)),
        ],
        cost_estimate=pl.CostEstimate(
            flops=half * 8 * eigvecs[0, 0].size * columns,
            bytes_accessed=eigvecs.size * 2,
            transcendentals=0,
        ),
        compiler_params=pltpu.CompilerParams(vmem_limit_bytes=16 << 20),
        name="project_partner" if partner else "project_own",
    )(
        pltpu.with_memory_space_constraint(eigvecs, pltpu.HBM),
        pltpu.with_memory_space_constraint(solutions, pltpu.HBM),
    )


def finish_kernel(scale, gathered, tau, tau_out, corr_out):
    corr_out[...] = jnp.sum(gathered[...], axis=(0, 1)) * scale
    tau_out[...] = tau[...]


def finish(gathered, tau, scale):
    return pl.pallas_call(
        functools.partial(finish_kernel, scale),
        out_shape=(
            jax.ShapeDtypeStruct(tau.shape, jnp.float32),
            jax.ShapeDtypeStruct(gathered.shape[-1:], jnp.float32),
        ),
        in_specs=[pl.BlockSpec(memory_space=pltpu.VMEM)] * 2,
        out_specs=[pl.BlockSpec(memory_space=pltpu.VMEM)] * 2,
        compiler_params=pltpu.CompilerParams(vmem_limit_bytes=16 << 20),
        name="finish",
    )(gathered, tau)


def shifted(array, axis, by):
    length = lax.axis_size(axis)
    return lax.ppermute(array, axis, [(i, (i + by) % length) for i in range(length)])


def block_at(blocks, index):
    return lax.dynamic_index_in_dim(blocks, index, 0, keepdims=False)


def sum_by_permutes(blocks, axis, me, order=(1, 2, 3)):
    length = lax.axis_size(axis)
    total = block_at(blocks, me)
    for by in order:
        total = total + shifted(block_at(blocks, (me + by) % length), axis, by)
    return total


def sum_by_swaps(blocks, axis, me, order=(1, 2, 3)):
    length = lax.axis_size(axis)
    total = block_at(blocks, me)
    for bits in order:
        swap = [(i, i ^ bits) for i in range(length)]
        total = total + lax.ppermute(block_at(blocks, me ^ bits), axis, swap)
    return total


def sum_by_all_to_all(blocks, axis):
    return jnp.sum(lax.all_to_all(blocks, axis, 0, 0, tiled=True), axis=0)


def per_device(eigvecs, solutions):
    zq, zp, y, core = (lax.axis_size(axis) for axis in SA)
    zh = zq * zp
    rows, columns = eigvecs.shape[-1], solutions.shape[-1]
    scale = 1.0 / (2.0 * rows * columns)
    slices = eigvecs.shape[0]
    half = slices // core
    block = rows // (zh * y)
    me, at_y, at_z = (lax.axis_index(axis) for axis in ("core", "y", ("zq", "zp")))
    ta = lax.axis_index("x") * lax.axis_size("zl") + lax.axis_index("zl")
    from_partner = shifted(project(eigvecs, solutions, True), "core", 1)
    tiles = project(eigvecs, solutions, False) + from_partner
    tiles = sum_by_swaps(tiles, "y", at_y, (2, 1, 3))
    total = tiles
    for bits in (2, 1, 3):
        total = total + lax.ppermute(tiles, ("zq", "zp"), [(i, i ^ bits) for i in range(zh)])
    every = jnp.sum(total * total, axis=(0, 2, 3))
    mine = block_at(total, at_z)
    squares = every
    pieces = jnp.moveaxis(mine.reshape(half * 2, core, block // core, columns), 1, 0)
    spare = jnp.zeros((block // core - half, columns), jnp.float32)
    packed = jnp.concatenate(
        [block_at(pieces, 1 - me), jnp.concatenate([squares, spare])[None]]
    )
    received = shifted(packed, "core", 1)

    def in_order(own, other):
        return jnp.where(me == 0, jnp.stack([own, other]), jnp.stack([other, own]))

    tau = in_order(block_at(pieces, me), received[:-1]).reshape(slices, 2, block // core, columns)
    norms = jnp.sum(in_order(squares, received[-1, :half]), axis=2).reshape(slices)
    spread = lax.axis_size("x") * lax.axis_size("zl")
    row = jnp.where(lax.iota(jnp.int32, spread)[:, None] == ta, norms[None], 0.0).reshape(-1)
    count = 1
    for axis in CHIPS:
        count *= lax.axis_size(axis)
    copies = jnp.broadcast_to(row, (count, 1, row.size))
    copies, tau = lax.optimization_barrier((copies, tau))
    gathered = lax.all_to_all(copies, CHIPS, split_axis=0, concat_axis=0, tiled=True)
    return finish(gathered, tau, scale)


def solution(mesh):
    fine = Mesh(mesh.devices.reshape(SIZES), AXES)
    in_specs = (P(TA, None, None, SA, None), P(TA, None, None, SA, None))
    out_specs = (P(TA, None, SA, None), P())
    return jax.shard_map(
        per_device, mesh=fine, in_specs=in_specs, out_specs=out_specs, check_vma=False
    )
```

```python
import functools

import jax
import jax.numpy as jnp
from jax import lax
from jax.experimental import pallas as pl
from jax.experimental.pallas import tpu as pltpu
from jax.sharding import Mesh, PartitionSpec as P

AXES = ("x", "zl", "zq", "zp", "y", "core")
SIZES = (4, 2, 2, 2, 4, 2)
TA = ("x", "zl")
SA = ("zq", "zp", "y", "core")
CHIPS = ("x", "zl", "y")


def project_kernel(partner, vecs, sols, out, vec_buf, sol_buf, sems):
    half = out.shape[2]
    owner = lax.axis_index("core")
    if partner:
        owner = 1 - owner
    copies = []
    for i in range(half):
        t = owner * half + i
        pair = [
            pltpu.make_async_copy(vecs.at[t], vec_buf.at[i], sems.at[0, i]),
            pltpu.make_async_copy(sols.at[t], sol_buf.at[i], sems.at[1, i]),
        ]
        for copy in pair:
            copy.start()
        copies.append(pair)
    ny, nz = out.shape[:2]
    rows = out.shape[4]
    for i in range(half):
        for copy in copies[i]:
            copy.wait()
        depth = vec_buf.shape[2] * vec_buf.shape[3]
        nev, nb = vec_buf.shape[-1], sol_buf.shape[-1]
        left = jnp.concatenate([vec_buf[i, p].reshape(depth, nev) for p in range(2)], 1)
        right = jnp.concatenate([sol_buf[i, p].reshape(depth, nb) for p in range(2)], 1)
        product = lax.dot_general(
            left, right, (((0,), (0,)), ((), ())), preferred_element_type=jnp.float32
        )
        real = product[:nev, :nb] + product[nev:, nb:]
        imag = product[:nev, nb:] - product[nev:, :nb]
        for z in range(nz):
            for y in range(ny):
                at = (z * ny + y) * rows
                out[y, z, i, 0] = real[at : at + rows]
                out[y, z, i, 1] = imag[at : at + rows]


def project(eigvecs, solutions, partner):
    zq, zp, y, core = (lax.axis_size(axis) for axis in SA)
    zh = zq * zp
    half = eigvecs.shape[0] // core
    rows = eigvecs.shape[-1] // (zh * y)
    columns = solutions.shape[-1]
    return pl.pallas_call(
        functools.partial(project_kernel, partner),
        out_shape=pltpu.VMEM((y, zh, half, 2, rows, columns), jnp.float32),
        in_specs=[pl.BlockSpec(memory_space=pltpu.HBM)] * 2,
        out_specs=pl.BlockSpec(memory_space=pltpu.VMEM),
        scratch_shapes=[
            pltpu.VMEM((half, *eigvecs.shape[1:]), eigvecs.dtype),
            pltpu.VMEM((half, *solutions.shape[1:]), solutions.dtype),
            pltpu.SemaphoreType.DMA((2, half)),
        ],
        cost_estimate=pl.CostEstimate(
            flops=half * 8 * eigvecs[0, 0].size * columns,
            bytes_accessed=eigvecs.size * 2,
            transcendentals=0,
        ),
        compiler_params=pltpu.CompilerParams(vmem_limit_bytes=16 << 20),
        name="project_partner" if partner else "project_own",
    )(
        pltpu.with_memory_space_constraint(eigvecs, pltpu.HBM),
        pltpu.with_memory_space_constraint(solutions, pltpu.HBM),
    )


def meet_kernel(pieces, squares, received, tau, copies):
    half = squares.shape[0]
    me = lax.axis_index("core")
    ta = lax.axis_index("x") * lax.axis_size("zl") + lax.axis_index("zl")
    slices = tau.shape[0]
    own, other = me * half, (1 - me) * half
    tau[pl.ds(own, half)] = pieces[me].reshape(half, *tau.shape[1:])
    tau[pl.ds(other, half)] = received[: 2 * half].reshape(half, *tau.shape[1:])
    lane = lax.broadcasted_iota(jnp.int32, (1, copies.shape[-1]), 1) - ta * slices
    row = jnp.zeros((1, copies.shape[-1]), jnp.float32)
    for at, lanes in ((own, squares[...]), (other, received[2 * half])):
        for i in range(half):
            norm = jnp.sum(lanes[i : i + 1], axis=1, keepdims=True)
            row = jnp.where(lane == at + i, norm, row)
    copies[...] = jnp.broadcast_to(row[None], copies.shape)


def meet(pieces, squares, received, slices, spread, count):
    half = squares.shape[0]
    core, _, rows, columns = pieces.shape
    return pl.pallas_call(
        meet_kernel,
        out_shape=[
            pltpu.VMEM((slices, 2, rows, columns), jnp.float32),
            pltpu.VMEM((count, 1, spread * slices), jnp.float32),
        ],
        in_specs=[pl.BlockSpec(memory_space=pltpu.VMEM)] * 3,
        out_specs=[pl.BlockSpec(memory_space=pltpu.VMEM)] * 2,
        compiler_params=pltpu.CompilerParams(vmem_limit_bytes=16 << 20),
        name="meet",
    )(pieces, squares, received)


def finish_kernel(scale, gathered, tau, tau_out, corr_out):
    corr_out[...] = jnp.sum(gathered[...], axis=(0, 1)) * scale
    tau_out[...] = tau[...]


def finish(gathered, tau, scale):
    return pl.pallas_call(
        functools.partial(finish_kernel, scale),
        out_shape=(
            jax.ShapeDtypeStruct(tau.shape, jnp.float32),
            jax.ShapeDtypeStruct(gathered.shape[-1:], jnp.float32),
        ),
        in_specs=[pl.BlockSpec(memory_space=pltpu.VMEM)] * 2,
        out_specs=[pl.BlockSpec(memory_space=pltpu.VMEM)] * 2,
        compiler_params=pltpu.CompilerParams(vmem_limit_bytes=16 << 20),
        name="finish",
    )(gathered, tau)


def shifted(array, axis, by):
    length = lax.axis_size(axis)
    return lax.ppermute(array, axis, [(i, (i + by) % length) for i in range(length)])


def block_at(blocks, index):
    return lax.dynamic_index_in_dim(blocks, index, 0, keepdims=False)


def sum_by_permutes(blocks, axis, me, order=(1, 2, 3)):
    length = lax.axis_size(axis)
    total = block_at(blocks, me)
    for by in order:
        total = total + shifted(block_at(blocks, (me + by) % length), axis, by)
    return total


def sum_by_swaps(blocks, axis, me, order=(1, 2, 3)):
    length = lax.axis_size(axis)
    total = block_at(blocks, me)
    for bits in order:
        swap = [(i, i ^ bits) for i in range(length)]
        total = total + lax.ppermute(block_at(blocks, me ^ bits), axis, swap)
    return total


def sum_by_all_to_all(blocks, axis):
    return jnp.sum(lax.all_to_all(blocks, axis, 0, 0, tiled=True), axis=0)


def per_device(eigvecs, solutions):
    zq, zp, y, core = (lax.axis_size(axis) for axis in SA)
    zh = zq * zp
    rows, columns = eigvecs.shape[-1], solutions.shape[-1]
    scale = 1.0 / (2.0 * rows * columns)
    slices = eigvecs.shape[0]
    half = slices // core
    block = rows // (zh * y)
    me, at_y, at_z = (lax.axis_index(axis) for axis in ("core", "y", ("zq", "zp")))
    from_partner = shifted(project(eigvecs, solutions, True), "core", 1)
    tiles = project(eigvecs, solutions, False) + from_partner
    tiles = sum_by_swaps(tiles, "y", at_y, (1, 3, 2))
    total = tiles
    for bits in (2, 1, 3):
        total = total + lax.ppermute(tiles, ("zq", "zp"), [(i, i ^ bits) for i in range(zh)])
    every = jnp.sum(total * total, axis=(0, 2, 3))
    mine = block_at(total, at_z)
    squares = every
    pieces = jnp.moveaxis(mine.reshape(half * 2, core, block // core, columns), 1, 0)
    spare = jnp.zeros((block // core - half, columns), jnp.float32)
    packed = jnp.concatenate(
        [block_at(pieces, 1 - me), jnp.concatenate([squares, spare])[None]]
    )
    received = shifted(packed, "core", 1)

    count = 1
    for axis in CHIPS:
        count *= lax.axis_size(axis)
    spread = lax.axis_size("x") * lax.axis_size("zl")
    tau, copies = meet(pieces, squares, received, slices, spread, count)
    gathered = lax.all_to_all(copies, CHIPS, split_axis=0, concat_axis=0, tiled=True)
    return finish(gathered, tau, scale)


def solution(mesh):
    fine = Mesh(mesh.devices.reshape(SIZES), AXES)
    in_specs = (P(TA, None, None, SA, None), P(TA, None, None, SA, None))
    out_specs = (P(TA, None, SA, None), P())
    return jax.shard_map(
        per_device, mesh=fine, in_specs=in_specs, out_specs=out_specs, check_vma=False
    )
```

```python
import functools

import jax
import jax.numpy as jnp
from jax import lax
from jax.experimental import pallas as pl
from jax.experimental.pallas import tpu as pltpu
from jax.sharding import Mesh, PartitionSpec as P

AXES = ("x", "zl", "zq", "zp", "y", "core")
SIZES = (4, 2, 2, 2, 4, 2)
TA = ("x", "zl")
SA = ("zq", "zp", "y", "core")
CHIPS = ("x", "zl", "y")


def project_kernel(partner, vecs, sols, out, vec_buf, sol_buf, sems):
    half = out.shape[2]
    owner = lax.axis_index("core")
    if partner:
        owner = 1 - owner
    copies = []
    for i in range(half):
        t = owner * half + i
        pair = [
            pltpu.make_async_copy(vecs.at[t], vec_buf.at[i], sems.at[0, i]),
            pltpu.make_async_copy(sols.at[t], sol_buf.at[i], sems.at[1, i]),
        ]
        for copy in pair:
            copy.start()
        copies.append(pair)
    ny, nz = out.shape[:2]
    rows = out.shape[4]
    for i in range(half):
        for copy in copies[i]:
            copy.wait()
        depth = vec_buf.shape[2] * vec_buf.shape[3]
        nev, nb = vec_buf.shape[-1], sol_buf.shape[-1]
        left = jnp.concatenate([vec_buf[i, p].reshape(depth, nev) for p in range(2)], 1)
        right = jnp.concatenate([sol_buf[i, p].reshape(depth, nb) for p in range(2)], 1)
        product = lax.dot_general(
            left, right, (((0,), (0,)), ((), ())), preferred_element_type=jnp.float32
        )
        real = product[:nev, :nb] + product[nev:, nb:]
        imag = product[:nev, nb:] - product[nev:, :nb]
        for z in range(nz):
            for y in range(ny):
                at = (z * ny + y) * rows
                out[y, z, i, 0] = real[at : at + rows]
                out[y, z, i, 1] = imag[at : at + rows]


def project(eigvecs, solutions, partner):
    zq, zp, y, core = (lax.axis_size(axis) for axis in SA)
    zh = zq * zp
    half = eigvecs.shape[0] // core
    rows = eigvecs.shape[-1] // (zh * y)
    columns = solutions.shape[-1]
    return pl.pallas_call(
        functools.partial(project_kernel, partner),
        out_shape=pltpu.VMEM((y, zh, half, 2, rows, columns), jnp.float32),
        in_specs=[pl.BlockSpec(memory_space=pltpu.HBM)] * 2,
        out_specs=pl.BlockSpec(memory_space=pltpu.VMEM),
        scratch_shapes=[
            pltpu.VMEM((half, *eigvecs.shape[1:]), eigvecs.dtype),
            pltpu.VMEM((half, *solutions.shape[1:]), solutions.dtype),
            pltpu.SemaphoreType.DMA((2, half)),
        ],
        cost_estimate=pl.CostEstimate(
            flops=half * 8 * eigvecs[0, 0].size * columns,
            bytes_accessed=eigvecs.size * 2,
            transcendentals=0,
        ),
        compiler_params=pltpu.CompilerParams(vmem_limit_bytes=16 << 20),
        name="project_partner" if partner else "project_own",
    )(
        pltpu.with_memory_space_constraint(eigvecs, pltpu.HBM),
        pltpu.with_memory_space_constraint(solutions, pltpu.HBM),
    )


def meet_kernel(pieces, squares, received, tau, copies):
    half = squares.shape[0]
    me = lax.axis_index("core")
    ta = lax.axis_index("x") * lax.axis_size("zl") + lax.axis_index("zl")
    slices = tau.shape[0]
    own, other = me * half, (1 - me) * half
    tau[pl.ds(own, half)] = pieces[me].reshape(half, *tau.shape[1:])
    tau[pl.ds(other, half)] = received[: 2 * half].reshape(half, *tau.shape[1:])
    lane = lax.broadcasted_iota(jnp.int32, (1, copies.shape[-1]), 1) - ta * slices
    row = jnp.zeros((1, copies.shape[-1]), jnp.float32)
    for at, lanes in ((own, squares[...]), (other, received[2 * half])):
        for i in range(half):
            norm = jnp.sum(lanes[i : i + 1], axis=1, keepdims=True)
            row = jnp.where(lane == at + i, norm, row)
    copies[...] = jnp.broadcast_to(row[None], copies.shape)


def meet(pieces, squares, received, slices, spread, count):
    half = squares.shape[0]
    core, _, rows, columns = pieces.shape
    return pl.pallas_call(
        meet_kernel,
        out_shape=[
            pltpu.VMEM((slices, 2, rows, columns), jnp.float32),
            pltpu.VMEM((count, 1, spread * slices), jnp.float32),
        ],
        in_specs=[pl.BlockSpec(memory_space=pltpu.VMEM)] * 3,
        out_specs=[pl.BlockSpec(memory_space=pltpu.VMEM)] * 2,
        compiler_params=pltpu.CompilerParams(vmem_limit_bytes=16 << 20),
        name="meet",
    )(pieces, squares, received)


def finish_kernel(scale, gathered, tau, tau_out, corr_out):
    corr_out[...] = jnp.sum(gathered[...], axis=(0, 1)) * scale
    tau_out[...] = tau[...]


def finish(gathered, tau, scale):
    return pl.pallas_call(
        functools.partial(finish_kernel, scale),
        out_shape=(
            jax.ShapeDtypeStruct(tau.shape, jnp.float32),
            jax.ShapeDtypeStruct(gathered.shape[-1:], jnp.float32),
        ),
        in_specs=[pl.BlockSpec(memory_space=pltpu.VMEM)] * 2,
        out_specs=[pl.BlockSpec(memory_space=pltpu.VMEM)] * 2,
        compiler_params=pltpu.CompilerParams(vmem_limit_bytes=16 << 20),
        name="finish",
    )(gathered, tau)


def shifted(array, axis, by):
    length = lax.axis_size(axis)
    return lax.ppermute(array, axis, [(i, (i + by) % length) for i in range(length)])


def block_at(blocks, index):
    return lax.dynamic_index_in_dim(blocks, index, 0, keepdims=False)


def sum_by_permutes(blocks, axis, me, order=(1, 2, 3)):
    length = lax.axis_size(axis)
    total = block_at(blocks, me)
    for by in order:
        total = total + shifted(block_at(blocks, (me + by) % length), axis, by)
    return total


def sum_by_swaps(blocks, axis, me, order=(1, 2, 3)):
    length = lax.axis_size(axis)
    total = block_at(blocks, me)
    for bits in order:
        swap = [(i, i ^ bits) for i in range(length)]
        total = total + lax.ppermute(block_at(blocks, me ^ bits), axis, swap)
    return total


def sum_by_all_to_all(blocks, axis):
    return jnp.sum(lax.all_to_all(blocks, axis, 0, 0, tiled=True), axis=0)


def per_device(eigvecs, solutions):
    zq, zp, y, core = (lax.axis_size(axis) for axis in SA)
    zh = zq * zp
    rows, columns = eigvecs.shape[-1], solutions.shape[-1]
    scale = 1.0 / (2.0 * rows * columns)
    slices = eigvecs.shape[0]
    half = slices // core
    block = rows // (zh * y)
    me, at_y, at_z = (lax.axis_index(axis) for axis in ("core", "y", ("zq", "zp")))
    from_partner = shifted(project(eigvecs, solutions, True), "core", 1)
    tiles = project(eigvecs, solutions, False) + from_partner
    total = block_at(tiles, at_y)
    for first, second in ((1, 3), (2, 2), (3, 1)):
        swap = [(i * core + c, (i ^ (first, second)[c]) * core + c) for i in range(y) for c in range(core)]
        sent = block_at(tiles, at_y ^ jnp.where(me == 0, first, second))
        total = total + lax.ppermute(sent, ("y", "core"), swap)
    tiles = total
    total = tiles
    for bits in (2, 1, 3):
        total = total + lax.ppermute(tiles, ("zq", "zp"), [(i, i ^ bits) for i in range(zh)])
    every = jnp.sum(total * total, axis=(0, 2, 3))
    mine = block_at(total, at_z)
    squares = every
    pieces = jnp.moveaxis(mine.reshape(half * 2, core, block // core, columns), 1, 0)
    spare = jnp.zeros((block // core - half, columns), jnp.float32)
    packed = jnp.concatenate(
        [block_at(pieces, 1 - me), jnp.concatenate([squares, spare])[None]]
    )
    received = shifted(packed, "core", 1)

    count = 1
    for axis in CHIPS:
        count *= lax.axis_size(axis)
    spread = lax.axis_size("x") * lax.axis_size("zl")
    tau, copies = meet(pieces, squares, received, slices, spread, count)
    gathered = lax.all_to_all(copies, CHIPS, split_axis=0, concat_axis=0, tiled=True)
    return finish(gathered, tau, scale)


def solution(mesh):
    fine = Mesh(mesh.devices.reshape(SIZES), AXES)
    in_specs = (P(TA, None, None, SA, None), P(TA, None, None, SA, None))
    out_specs = (P(TA, None, SA, None), P())
    return jax.shard_map(
        per_device, mesh=fine, in_specs=in_specs, out_specs=out_specs, check_vma=False
    )
```
